512 devices in a mesh: cx: 16 (over z_hi, y), cy: 32 (over x, z_lo, core).
Axes of the slice: x: 4, y: 8, z: 8 (z_hi: 2, z_lo: 4; z = z_hi * 4 + z_lo), core: 2. Of those that a mesh axis runs over, the one named last changes fastest.
Arguments:
- queries: bfloat16 [7, 32768, 128], P(None, ('cx', 'cy')), may hold values from -8 to 8, as said below
- keys: bfloat16 [32768, 128], P(('cx', 'cy')), may hold values from -40 to 40, as said below
- values: bfloat16 [32768, 128], P(('cx', 'cy')), may hold values from -6 to 6
Outputs:
- attended: bfloat16 [7, 32768, 128], P(None, ('cx', 'cy'))
The draws below stay inside these ranges and needn't reach their ends.
Inputs may be any that keep to these rules, and one draw needn't show every extreme that they name: `queries`: every query is noise of about unit size in each entry plus one common direction of length 4, the same for all heads and tokens. The keys of the first four prompt positions carry a large component along the queries' common direction, so they draw much of every query's attention; all other keys are noise of about unit size in each entry.
All inputs are finite; a program needn't handle non-finite values.
Results may differ from the reference program's by a relative error of at most 0.001.
Values may be sent and summed in bfloat16 or wider, within the bound.
A program may use at most 192 MiB of HBM per device.

```python
import math
import jax
import jax.numpy as jnp
from jax import lax

HEAD = 128
GROUP = 7
TOK_DEV = 64
SEQ = 32768


def sink_direction(key):
    sample = jax.random.normal(jax.random.fold_in(key, 3), (HEAD,), jnp.float32)
    return sample / jnp.sqrt(jnp.sum(sample * sample))


def noise_field(key, shape):
    return jnp.clip(jax.random.normal(key, shape, jnp.float32), -4.0, 4.0)


def draw_queries(key, part):
    direction = sink_direction(key)
    noise = noise_field(jax.random.fold_in(key, 1), (GROUP, SEQ, HEAD))
    return (noise + 4.0 * direction).astype(jnp.bfloat16)


def draw_keys(key, part):
    direction = sink_direction(key)
    noise = noise_field(jax.random.fold_in(key, 2), (SEQ, HEAD))
    lift = math.sqrt(HEAD) * (math.log(SEQ) - 1.0) / 4.0
    sinks = (jnp.arange(SEQ) < 4).astype(jnp.float32)
    return (noise + lift * sinks[:, None] * direction[None, :]).astype(jnp.bfloat16)


def block_scale(own_key, dims, shards, least, top_value):
    def one(position, parts):
        heights = jax.random.uniform(jax.random.fold_in(jax.random.fold_in(own_key, 6), position), (parts,), jnp.float32, least / len(shards), top_value / len(shards))
        return jnp.repeat(jnp.exp(heights), dims[position] // parts).reshape((-1,) + (1,) * (len(dims) - position - 1))

    level = one(*shards[0])
    for cut in shards[1:]:
        level = level * one(*cut)
    return level


def normal_values(rng, shape, spread, reach, pieces=(), kind=jnp.bfloat16):
    values = spread * jax.random.normal(rng, shape, jnp.float32)
    if pieces:
        values = values * block_scale(rng, shape, pieces, -0.22, 0.18)
    return jnp.clip(values, -reach, reach).astype(kind)


def setup_inputs(seed: int = 0) -> dict:
    key_of = jax.random.split(jax.random.key(seed), 4)
    return {
        "queries": draw_queries(jax.random.fold_in(key_of[3], 71), 0),
        "keys": draw_keys(jax.random.fold_in(key_of[3], 71), 0),
        "values": normal_values(key_of[2], (SEQ, HEAD), 1.0, 6.0, ((0, 512),)),
    }


masked = -1e30


def reference(queries, keys, values):
    key_pos = jnp.arange(SEQ, dtype=jnp.int32)
    values_wide = values.astype(jnp.float32)

    def row_block(number):
        first = (number * TOK_DEV).astype(jnp.int32)
        chosen = lax.dynamic_slice_in_dim(queries, first, TOK_DEV, 1).reshape(GROUP * TOK_DEV, HEAD)
        query_pos = first + jnp.arange(GROUP * TOK_DEV, dtype=jnp.int32) % TOK_DEV
        scores = jnp.dot(chosen, keys.T, preferred_element_type=jnp.float32) * (HEAD ** -0.5)
        visible = key_pos[None, :] <= query_pos[:, None]
        scores = jnp.where(visible, scores, masked)
        peak = jnp.max(scores, axis=1, keepdims=True)
        weights = jnp.where(visible, jnp.exp(scores - peak), 0.0)
        total = jnp.sum(weights, axis=1, keepdims=True)
        mixed = jnp.dot(weights, values_wide, precision=lax.Precision.HIGHEST)
        return (mixed / total).astype(jnp.bfloat16).reshape(GROUP, TOK_DEV, HEAD)

    blocks = lax.map(row_block, jnp.arange(SEQ // TOK_DEV, dtype=jnp.int32))
    return jnp.transpose(blocks, (1, 0, 2, 3)).reshape(GROUP, SEQ, HEAD)
```

```python
import functools
import jax
import jax.numpy as jnp
from jax import lax
from jax.experimental import pallas as pl
from jax.experimental.pallas import tpu as pltpu
from jax.sharding import Mesh
from jax.sharding import PartitionSpec as P

AXES = ("zh", "y", "x", "zl", "core")
SIZES = (2, 8, 4, 4, 2)
SCALE = 128 ** -0.5
C2 = SCALE * 1.4426950408889634
F32 = jnp.float32
BF16 = jnp.bfloat16


def here():
    return tuple(lax.axis_index(name) for name in AXES)


def place_of(zh, y, x, zl, core):
    return ((((zh * 8 + y) * 4 + x) * 4 + zl) * 2 + core) * 64


def dot(a, b, dims):
    return lax.dot_general(a, b, (dims, ((), ())), preferred_element_type=F32)


def query_place(zh, y, zl, core):
    tile = lax.broadcasted_iota(jnp.int32, (7, 1, 256), 0)
    lane = lax.broadcasted_iota(jnp.int32, (7, 1, 256), 2)
    group = tile * 2 + lane // 128
    mate = jnp.where(group >= 7, 2, 0) + (lane % 128) // 64
    return place_of(zh, y, mate, zl, core) + lane % 64


def unit_facts(unit, x):
    late = unit >= 16
    v = unit - jnp.where(late, 16, 0)
    zh0, y0 = v % 2, v // 2
    zh1, zl1, y1 = v // 8, (v // 2) % 4, (v % 2) * 4
    first = jnp.where(late, place_of(zh1, y1, x, zl1, 1), place_of(zh0, y0, x, 0, 0))
    stride = jnp.where(late, 4 * 4 * 2 * 64, 2 * 64)
    low = jnp.where(late, zh1 * 8 + y1, zh0 * 8 + y0)
    high = jnp.where(late, low + 3, low)
    return first, stride, low, high


def compute_unit(unit, masked, facts, kv_ref, qt_ref, place_ref, shift_ref, ot_ref, sum_ref):
    first, stride = facts
    k = kv_ref[pl.ds(unit * 4, 4), 0].reshape(256, 128)
    vt = kv_ref[pl.ds(unit * 4, 4), 1].reshape(256, 128).T
    if masked:
        row = lax.broadcasted_iota(jnp.int32, (256, 256), 0)
        place = first + (row // 64) * stride + row % 64
    for t in range(7):
        s = dot(k, qt_ref[t], ((1,), (0,)))
        e = s * C2 - shift_ref[t]
        if masked:
            e = jnp.where((place <= place_ref[t]) & (place >= 64), e, -1e30)
        p = jnp.exp2(e)
        sum_ref[t] += p.reshape(32, 8, 256).sum(axis=0)
        ot_ref[t] += dot(vt, p.astype(BF16), ((1,), (0,)))


def attend_kernel(kv_ref, q_ref, own_ref, o_ref, stat_ref, qt_ref, place_ref, shift_ref, ot_ref, sum_ref):
    zh, y, x, zl, core = here()
    cx = zh * 8 + y
    place_ref[...] = query_place(zh, y, zl, core)
    ot_ref[...] = jnp.zeros_like(ot_ref)
    sum_ref[...] = jnp.zeros_like(sum_ref)
    for t in range(7):
        qt_ref[t] = q_ref[pl.ds(2 * t, 2)].reshape(256, 128).T
        s = dot(own_ref[0], qt_ref[t], ((1,), (0,)))
        shift_ref[t] = jnp.max(s, axis=0, keepdims=True) * C2

    def step(unit, carry):
        first, stride, low, high = unit_facts(unit, x)
        clear = (high < cx) & (unit > 0)

        @pl.when(clear)
        def _():
            compute_unit(unit, False, (first, stride), kv_ref, qt_ref, place_ref, shift_ref, ot_ref, sum_ref)

        @pl.when((low <= cx) & jnp.logical_not(clear))
        def _():
            compute_unit(unit, True, (first, stride), kv_ref, qt_ref, place_ref, shift_ref, ot_ref, sum_ref)

        return carry

    lax.fori_loop(0, 32, step, 0)
    for t in range(7):
        o_ref[pl.ds(2 * t, 2)] = ot_ref[t].T.reshape(2, 128, 128).astype(BF16)
        stat_ref[0, t] = shift_ref[t]
        stat_ref[1, t] = jnp.sum(sum_ref[t], axis=0, keepdims=True)


def attend(kv, q, own):
    vmem = pl.BlockSpec(memory_space=pltpu.VMEM)
    return pl.pallas_call(
        attend_kernel,
        out_shape=(
            jax.ShapeDtypeStruct((14, 128, 128), BF16),
            jax.ShapeDtypeStruct((2, 7, 1, 256), F32),
        ),
        in_specs=[vmem] * 3,
        out_specs=(vmem, vmem),
        scratch_shapes=[
            pltpu.VMEM((7, 128, 256), BF16),
            pltpu.VMEM((7, 1, 256), jnp.int32),
            pltpu.VMEM((7, 1, 256), F32),
            pltpu.VMEM((7, 128, 256), F32),
            pltpu.VMEM((7, 8, 256), F32),
        ],
        compiler_params=pltpu.CompilerParams(vmem_limit_bytes=48 * 1024 * 1024),
    )(kv, q, own)


def per_device(queries, keys, values):
    zh, y, x, zl, core = here()
    own = jnp.stack([keys, values])
    plane = lax.all_gather(own, ("zh", "y", "zl", "core"))
    plane = plane.reshape(2, 8, 4, 2, 2, 64, 128)
    first = plane[:, :, :, 0].transpose(1, 0, 2, 3, 4, 5).reshape(64, 2, 64, 128)
    second = plane[:, :, :, 1].transpose(0, 2, 1, 3, 4, 5).reshape(64, 2, 64, 128)
    kv = jnp.concatenate([first, second])
    q = lax.all_gather(queries, "x").reshape(2, 2, 7, 64, 128)
    q = q.transpose(0, 2, 1, 3, 4).reshape(14, 128, 128)
    o, stat = attend(kv, q, own)
    o = o.reshape(2, 7, 2, 64, 128).transpose(0, 2, 1, 3, 4).reshape(4, 448, 128)
    stat = stat.reshape(2, 2, 7, 2, 64).transpose(1, 3, 0, 2, 4).reshape(4, 2, 448)
    o = lax.all_to_all(o, "x", 0, 0)
    stat = lax.all_to_all(stat, "x", 0, 0)
    head = lax.all_gather(kv[0], "x")[0]
    flat = queries.reshape(448, 128)
    s = jnp.dot(flat, head[0].T, preferred_element_type=F32) * C2
    place = place_of(zh, y, x, zl, core) + jnp.arange(448) % 64
    seen = jnp.arange(64)[None, :] <= place[:, None]
    s = jnp.where(seen, s, -1e30)
    top = jnp.maximum(jnp.max(s, axis=1), jnp.max(stat[:, 0], axis=0))
    w = jnp.where(seen, jnp.exp2(s - top[:, None]), 0.0)
    high = w.astype(BF16)
    low = (w - high.astype(F32)).astype(BF16)
    mixed = jnp.dot(high, head[1], preferred_element_type=F32) + jnp.dot(low, head[1], preferred_element_type=F32)
    total = jnp.sum(w, axis=1)
    for n in range(4):
        scale = jnp.exp2(stat[n, 0] - top)
        mixed = mixed + o[n].astype(F32) * scale[:, None]
        total = total + stat[n, 1] * scale
    return (mixed / total[:, None]).astype(BF16).reshape(7, 64, 128)


def solution(mesh):
    split = Mesh(mesh.devices.reshape(SIZES), AXES)
    return jax.shard_map(
        per_device,
        mesh=split,
        in_specs=(P(None, AXES, None), P(AXES, None), P(AXES, None)),
        out_specs=P(None, AXES, None),
        check_vma=False,
    )
```
